32 devices in a mesh: gx: 4 (over y, x), gy: 8 (over z, core).
Axes of the slice: x: 2, y: 2, z: 4, core: 2. Of those that a mesh axis runs over, the one named last changes fastest.
Arguments:
- voltages: bfloat16 [2, 2048, 122880], P(None, ('gx', 'gy')), may hold values from -6 to 6
- gains: float32 [2, 2048, 8192], P(None, ('gx', 'gy')), may hold values from -6 to 6
- delays: float32 [64, 2048], replicated, may hold values from -32 to 32
- channel_order: int32 [4, 8], replicated, may hold values from 0 to 7, each once within a row
- beam_table: int32 [64], replicated, may hold values from 0 to 63, each once
Outputs:
- beam_power: float32 [64, 4, 8192], P('gy', None, 'gx')
The draws below stay inside these ranges and needn't reach their ends.
Inputs may be any that keep to these rules, and one draw needn't show every extreme that they name: Each row names every index of gy once; channel block a * 8 + channel_order[a, b] of 256 channels belongs to the device at gx = a, gy = b. Names every beam once; the beams beam_table[g * 64 / 8] onward, 64 / 8 of them, belong to gy index g.
All inputs are finite; a program needn't handle non-finite values.
Results may differ from the reference program's by a relative error of at most 0.009.
Values may be sent and summed in bfloat16 or wider, within the bound.
No kernel may reach another device: no remote copies, remote signals or barrier semaphores. Data moves between devices by JAX's collectives and lax.ppermute only.
A program may use at most 192 MiB of HBM per device.

```python
import math
import jax
import jax.numpy as jnp
from jax import lax

NIN = 2048
NCH = 8192
NBEAM = 64
TAPS = 8
INTEG = 2
NSPEC = 8
SAMPLES = 122880
TIMES = 4
N_GX = 4
N_GY = 8


def levels(own_key, shape, pieces, low, top_value):
    gain = 1.0
    for axis_at, shards_of in pieces:
        heights = jax.random.uniform(jax.random.fold_in(jax.random.fold_in(own_key, 6), axis_at), (shards_of,), jnp.float32, low / len(pieces), top_value / len(pieces))
        gain = gain * jnp.repeat(jnp.exp(heights), shape[axis_at] // shards_of).reshape((-1,) + (1,) * (len(shape) - 1 - axis_at))
    return gain


def gaussian(rng, dims, spread, most, split=(), kind=jnp.bfloat16):
    array = jax.random.normal(rng, dims, jnp.float32) * spread
    if len(split) > 0:
        array = levels(rng, dims, split, -0.22, 0.18) * array
    return jnp.clip(array, min=-most, max=most).astype(kind)


def setup_inputs(seed: int = 0) -> dict:
    splits = jax.random.split(jax.random.key(seed), 6)
    voltages = gaussian(splits[0], (2, NIN, SAMPLES), 1.0, 6.0, ((1, 32),))
    gains = gaussian(splits[1], (2, NIN, NCH), 1.0, 6.0, ((1, 32),), jnp.float32)
    delays = jnp.clip(jax.random.uniform(splits[2], (NBEAM, NIN), jnp.float32, -32.0, 32.0), -32.0, 32.0)
    channel_order = jax.vmap(lambda own: jax.random.permutation(own, N_GY))(jax.random.split(splits[3], N_GX)).reshape((N_GX, N_GY)).astype(jnp.int32)
    beam_table = jax.random.permutation(splits[4], NBEAM).astype(jnp.int32)
    return {"voltages": voltages, "gains": gains, "delays": delays, "channel_order": channel_order, "beam_table": beam_table}


def coefficients():
    total = TAPS * NCH
    index = jnp.arange(total, dtype=jnp.float32)
    offset = (index - total / 2) / NCH
    window = 0.5 - 0.5 * jnp.cos(2.0 * math.pi * index / total)
    raw = jnp.sinc(offset) * window
    raw = raw / jnp.sqrt(jnp.sum(raw * raw) / NCH)
    return raw.reshape(TAPS, NCH)

def transform(filtered):
    highest = lax.Precision.HIGHEST
    first_len = 64
    second_len = NCH // first_len
    first_ids = jnp.arange(first_len, dtype=jnp.int32)
    second_ids = jnp.arange(second_len, dtype=jnp.int32)
    small_angle = 2.0 * math.pi / first_len * (first_ids[:, None] * first_ids[None, :] % first_len).astype(jnp.float32)
    small_cos = jnp.cos(small_angle)
    small_sin = -jnp.sin(small_angle)
    small_stack = jnp.concatenate([jnp.concatenate([small_cos, -small_sin], axis=1), jnp.concatenate([small_sin, small_cos], axis=1)], axis=0)
    small_stack = small_stack.astype(jnp.bfloat16).astype(jnp.float32)
    twist_angle = 2.0 * math.pi / NCH * (first_ids[:, None] * second_ids[None, :]).astype(jnp.float32)
    twist_cos = jnp.cos(twist_angle)
    twist_sin = -jnp.sin(twist_angle)
    large_angle = 2.0 * math.pi / second_len * (second_ids[:, None] * second_ids[None, :] % second_len).astype(jnp.float32)
    large_cos = jnp.cos(large_angle)
    large_sin = -jnp.sin(large_angle)
    large_stack = jnp.concatenate([jnp.concatenate([large_cos, large_sin], axis=1), jnp.concatenate([-large_sin, large_cos], axis=1)], axis=0)
    large_stack = large_stack.astype(jnp.bfloat16).astype(jnp.float32)
    inputs_here = filtered.shape[1]
    spectra_here = filtered.shape[2]
    stacked = jnp.transpose(filtered.reshape(2, inputs_here, spectra_here, first_len, second_len), (1, 2, 0, 3, 4)).reshape(inputs_here, spectra_here, 2 * first_len, second_len).astype(jnp.float32)
    inner = jnp.einsum('km,ismq->iskq', small_stack, stacked, precision=highest)
    inner_real = inner[:, :, :first_len]
    inner_imag = inner[:, :, first_len:]
    turned_real = inner_real * twist_cos - inner_imag * twist_sin
    turned_imag = inner_real * twist_sin + inner_imag * twist_cos
    turned = jnp.concatenate([turned_real, turned_imag], axis=3).astype(jnp.bfloat16).astype(jnp.float32)
    outer = jnp.einsum('iskq,qn->isnk', turned, large_stack, precision=highest)
    scale = NCH ** (-0.5)
    outer_real = outer[:, :, :second_len].reshape(inputs_here, spectra_here, NCH) * scale
    outer_imag = outer[:, :, second_len:].reshape(inputs_here, spectra_here, NCH) * scale
    return (outer_real, outer_imag)

def reference(voltages, gains, delays, channel_order, beam_table):
    taps_table = coefficients()

    def channelize(inputs):
        samples, calib = inputs
        frames = samples.reshape(2, NSPEC + TAPS - 1, NCH)
        filtered = taps_table[0] * frames[:, 0:NSPEC].astype(jnp.float32)
        for tap_index in range(1, TAPS):
            filtered = filtered + taps_table[tap_index] * frames[:, tap_index:tap_index + NSPEC].astype(jnp.float32)
        filtered = filtered.astype(jnp.bfloat16)
        spec_real, spec_imag = transform(filtered[:, None])
        spec_real = spec_real[0]
        spec_imag = spec_imag[0]
        out_real = calib[0] * spec_real - calib[1] * spec_imag
        out_imag = calib[0] * spec_imag + calib[1] * spec_real
        return jnp.stack([out_real, out_imag]).astype(jnp.bfloat16)
    spectra = lax.map(channelize, (jnp.moveaxis(voltages, 1, 0), jnp.moveaxis(gains, 1, 0)))
    offsets = jnp.take(delays, beam_table, axis=0)
    block_channels = 64
    scale = NIN ** (-0.5)

    def beam_group(group_index):
        start = group_index * block_channels
        piece = lax.dynamic_slice_in_dim(spectra, start, block_channels, 3).astype(jnp.float32)
        channel = (start + jnp.arange(block_channels, dtype=jnp.int32)).astype(jnp.float32)
        phase = channel[:, None, None] * offsets[None] * (-2.0 * math.pi / NCH)
        weight_real = (jnp.cos(phase) * scale).astype(jnp.bfloat16).astype(jnp.float32)
        weight_imag = (jnp.sin(phase) * scale).astype(jnp.bfloat16).astype(jnp.float32)
        first = jnp.einsum('cbi,ipsc->cbps', weight_real, piece)
        second = jnp.einsum('cbi,ipsc->cbps', weight_imag, piece)
        beam_real = (first[:, :, 0] - second[:, :, 1]).astype(jnp.bfloat16).astype(jnp.float32)
        beam_imag = (first[:, :, 1] + second[:, :, 0]).astype(jnp.bfloat16).astype(jnp.float32)
        power = beam_real * beam_real + beam_imag * beam_imag
        return power.reshape(block_channels, NBEAM, TIMES, INTEG).sum(axis=3)
    groups = lax.map(beam_group, jnp.arange(NCH // block_channels, dtype=jnp.int32))
    natural = jnp.transpose(groups.reshape(NCH, NBEAM, TIMES), (1, 2, 0))
    devices = N_GX * N_GY
    width = NCH // devices
    order = (jnp.arange(N_GX, dtype=jnp.int32)[:, None] * N_GY + channel_order).reshape(-1)
    placed = jnp.take(natural.reshape(NBEAM, TIMES, devices, width), order, axis=2)
    return placed.reshape(NBEAM, TIMES, NCH)
```

```python
import functools
import math

import jax
import jax.numpy as jnp
from jax import lax
from jax.experimental import pallas as pl
from jax.experimental.pallas import tpu as pltpu
from jax.sharding import PartitionSpec as P

NIN = 2048
NCH = 8192
NBEAM = 64
TAPS = 8
INTEG = 2
NSPEC = 8
TIMES = 4
SLOT = 64
RUN = 64
COARSE = 16


def coefficients():
    total = TAPS * NCH
    index = jnp.arange(total, dtype=jnp.float32)
    offset = (index - total / 2) / NCH
    window = 0.5 - 0.5 * jnp.cos(2.0 * math.pi * index / total)
    raw = jnp.sinc(offset) * window
    raw = raw / jnp.sqrt(jnp.sum(raw * raw) / NCH)
    return raw.reshape(TAPS, NCH)


def transform(filtered):
    first_len = 64
    second_len = NCH // first_len
    first_ids = jnp.arange(first_len, dtype=jnp.int32)
    second_ids = jnp.arange(second_len, dtype=jnp.int32)
    small_angle = (
        2.0
        * math.pi
        / first_len
        * (first_ids[:, None] * first_ids[None, :] % first_len).astype(jnp.float32)
    )
    small_cos = jnp.cos(small_angle)
    small_sin = -jnp.sin(small_angle)
    small_stack = jnp.concatenate(
        [
            jnp.concatenate([small_cos, -small_sin], axis=1),
            jnp.concatenate([small_sin, small_cos], axis=1),
        ],
        axis=0,
    ).astype(jnp.bfloat16)
    twist_angle = (
        2.0 * math.pi / NCH * (first_ids[:, None] * second_ids[None, :]).astype(jnp.float32)
    )
    twist_cos = jnp.cos(twist_angle)
    twist_sin = -jnp.sin(twist_angle)
    large_angle = (
        2.0
        * math.pi
        / second_len
        * (second_ids[:, None] * second_ids[None, :] % second_len).astype(jnp.float32)
    )
    large_cos = jnp.cos(large_angle)
    large_sin = -jnp.sin(large_angle)
    large_stack = jnp.concatenate(
        [
            jnp.concatenate([large_cos, large_sin], axis=1),
            jnp.concatenate([-large_sin, large_cos], axis=1),
        ],
        axis=0,
    ).astype(jnp.bfloat16)
    inputs_here = filtered.shape[1]
    spectra_here = filtered.shape[2]
    stacked = jnp.transpose(
        filtered.reshape(2, inputs_here, spectra_here, first_len, second_len), (1, 2, 0, 3, 4)
    ).reshape(inputs_here, spectra_here, 2 * first_len, second_len)
    inner = jnp.einsum("km,ismq->iskq", small_stack, stacked, preferred_element_type=jnp.float32)
    inner_real = inner[:, :, :first_len]
    inner_imag = inner[:, :, first_len:]
    turned_real = inner_real * twist_cos - inner_imag * twist_sin
    turned_imag = inner_real * twist_sin + inner_imag * twist_cos
    turned = jnp.concatenate([turned_real, turned_imag], axis=3).astype(jnp.bfloat16)
    outer = jnp.einsum("iskq,qn->isnk", turned, large_stack, preferred_element_type=jnp.float32)
    scale = NCH ** (-0.5)
    outer_real = outer[:, :, :second_len].reshape(inputs_here, spectra_here, NCH) * scale
    outer_imag = outer[:, :, second_len:].reshape(inputs_here, spectra_here, NCH) * scale
    return (outer_real, outer_imag)


def spectra_of(voltages, gains):
    inputs_here = voltages.shape[1]
    frames = voltages.reshape(2, inputs_here, NSPEC + TAPS - 1, NCH)
    taps_table = coefficients()
    filtered = taps_table[0] * frames[:, :, 0:NSPEC].astype(jnp.float32)
    for tap_index in range(1, TAPS):
        filtered = filtered + taps_table[tap_index] * frames[
            :, :, tap_index : tap_index + NSPEC
        ].astype(jnp.float32)
    spec_real, spec_imag = transform(filtered.astype(jnp.bfloat16))
    gain_real = gains[0][:, None, :]
    gain_imag = gains[1][:, None, :]
    calibrated = jnp.stack(
        [
            gain_real * spec_real - gain_imag * spec_imag,
            gain_real * spec_imag + gain_imag * spec_real,
        ]
    ).astype(jnp.bfloat16)
    arranged = jnp.transpose(calibrated, (3, 2, 0, 1))
    if inputs_here < SLOT:
        arranged = jnp.pad(arranged, ((0, 0), (0, 0), (0, 0), (0, SLOT - inputs_here)))
    return arranged.reshape(NCH, NSPEC, 2 * SLOT)


def phase_tables(offsets):
    turn = offsets * (2.0 * math.pi / NCH)
    both = jnp.concatenate([turn, turn], axis=1)
    fine = jnp.arange(RUN, dtype=jnp.float32)[:, None, None] * both[None]
    steps = NCH // RUN // COARSE
    middle = (RUN * jnp.arange(COARSE, dtype=jnp.float32))[:, None, None] * both[None]
    wide = (RUN * COARSE * jnp.arange(steps, dtype=jnp.float32))[:, None, None] * turn[None]
    wide_cos = jnp.cos(wide)
    wide_sin = jnp.sin(wide)
    scale = NIN ** (-0.5)
    return (
        jnp.stack([jnp.cos(fine), jnp.sin(fine)]),
        jnp.stack([jnp.cos(middle), jnp.sin(middle)]),
        jnp.stack(
            [
                jnp.concatenate([wide_cos, wide_sin], axis=2) * scale,
                jnp.concatenate([wide_sin, -wide_cos], axis=2) * scale,
            ]
        ),
    )


def beam_kernel(spectra, fine, middle, wide, out):
    step = pl.program_id(0)
    lanes = 2 * SLOT
    bases = []
    for half in range(2):
        run = 2 * step + half
        coarse = run // COARSE
        rest = run % COARSE
        wide_cos = wide[0, coarse]
        wide_sin = wide[1, coarse]
        middle_cos = middle[0, rest]
        middle_sin = middle[1, rest]
        bases.append(
            (
                wide_cos * middle_cos - wide_sin * middle_sin,
                wide_sin * middle_cos + wide_cos * middle_sin,
            )
        )
    lane = lax.broadcasted_iota(jnp.int32, (NBEAM, 2 * lanes), 1)
    member = (lane // NSPEC) % 8
    sign = jnp.where(
        lax.broadcasted_iota(jnp.int32, (8 * NSPEC, lanes), 1) < SLOT, 1.0, -1.0
    ).astype(jnp.float32)
    blank = jnp.zeros((16 * NSPEC, lanes), jnp.bfloat16)

    def group(index):
        rights = []
        for half in range(2):
            block = spectra[half, pl.ds(index * 8, 8)].reshape(8 * NSPEC, lanes)
            swapped = (pltpu.roll(block.astype(jnp.float32), SLOT, 1) * sign).astype(jnp.bfloat16)
            rights.append(jnp.concatenate([block, swapped], axis=0))
        right = jnp.concatenate(
            [
                jnp.concatenate([rights[0], blank], axis=1),
                jnp.concatenate([blank, rights[1]], axis=1),
            ],
            axis=0,
        )
        lefts = []
        for inner in range(8):
            fine_cos = fine[0, index * 8 + inner]
            fine_sin = fine[1, index * 8 + inner]
            lefts.append(
                jnp.concatenate(
                    [
                        (base_cos * fine_cos - base_sin * fine_sin).astype(jnp.bfloat16)
                        for base_cos, base_sin in bases
                    ],
                    axis=1,
                )
            )
        products = lax.dot_general(
            jnp.concatenate(lefts, axis=0),
            right,
            (((1,), (1,)), ((), ())),
            preferred_element_type=jnp.float32,
        )
        total = products[:NBEAM]
        for inner in range(1, 8):
            total = jnp.where(
                member == inner, products[inner * NBEAM : (inner + 1) * NBEAM], total
            )
        return total

    def pair(index, carry):
        low = group(2 * index)
        high = group(2 * index + 1)
        for unit in range(8):
            rows = slice(unit * 8, unit * 8 + 8)
            both = jnp.concatenate([low[rows], high[rows]], axis=0).astype(jnp.bfloat16)
            out[unit % 2, 0, unit // 2, pl.ds(index * 16, 16), :] = both
        return carry

    lax.fori_loop(0, RUN // 16, pair, 0)


def partial_beams(spectra, tables):
    runs = NCH // (2 * RUN)
    fine, middle, wide = tables
    whole = lambda array: pl.BlockSpec(array.shape, lambda step: (0,) * array.ndim)
    return pl.pallas_call(
        beam_kernel,
        grid=(runs,),
        in_specs=[
            pl.BlockSpec((2, RUN, NSPEC, 2 * SLOT), lambda step: (step, 0, 0, 0)),
            whole(fine),
            whole(middle),
            whole(wide),
        ],
        out_specs=pl.BlockSpec((2, 1, 4, RUN, 4 * SLOT), lambda step: (0, step, 0, 0, 0)),
        out_shape=jax.ShapeDtypeStruct((2, runs, 4, RUN, 4 * SLOT), jnp.bfloat16),
        compiler_params=pltpu.CompilerParams(
            dimension_semantics=("arbitrary",), vmem_limit_bytes=48 * 1024 * 1024
        ),
        name="beam_sums",
    )(spectra.reshape(NCH // RUN, RUN, NSPEC, 2 * SLOT), fine, middle, wide)


def detect(beams):
    runs, groups, count, lanes = beams.shape
    wide = beams.astype(jnp.float32)
    source = jnp.arange(lanes, dtype=jnp.int32)
    source_half = source // (16 * NSPEC)
    source_channel = source // NSPEC % 8
    source_time = source % NSPEC // INTEG
    place = (source_half * TIMES + source_time) * 8 + source_channel
    pick = (place[:, None] == jnp.arange(2 * TIMES * 8, dtype=jnp.int32)[None]).astype(jnp.float32)
    power = jnp.einsum(
        "tgrl,lm->tgrm",
        wide * wide,
        pick,
        precision=lax.Precision.HIGHEST,
        preferred_element_type=jnp.float32,
    )
    power = power.reshape(runs, groups, count, 2, TIMES, 8)
    return jnp.transpose(power, (2, 4, 0, 3, 1, 5)).reshape(count, TIMES, runs * 2 * groups * 8)


def body(voltages, gains, delays, channel_order, beam_table):
    across = lax.axis_size("gx")
    along = lax.axis_size("gy")
    inputs_here = voltages.shape[1]
    beams_here = NBEAM // along
    column = lax.axis_index("gx")
    member = lax.axis_index("gy")
    first_input = (column * along + member) * inputs_here
    offsets = jnp.take(
        lax.dynamic_slice_in_dim(delays, first_input, inputs_here, 1), beam_table, axis=0
    )
    if inputs_here < SLOT:
        offsets = jnp.pad(offsets, ((0, 0), (0, SLOT - inputs_here)))
    spectra = spectra_of(voltages, gains)
    partial = partial_beams(spectra, phase_tables(offsets))
    runs = partial.shape[1]
    groups = RUN // 8
    lanes = 4 * SLOT
    pairs = [[2 * index, 2 * index + 1] for index in range(along // 2)]
    evens = [[2 * index + odd for index in range(along // 2)] for odd in range(2)]
    if beams_here != 8:
        partial = jnp.transpose(
            partial.reshape(2, runs, 4, groups, 8, lanes), (2, 0, 4, 1, 3, 5)
        ).reshape(along // 2, 2, beams_here, runs, groups, lanes)
        partial = jnp.transpose(partial, (1, 3, 0, 4, 2, 5)).reshape(
            2, runs, along // 2, groups * beams_here, lanes
        )
    halves = lax.all_to_all(partial, "gy", 0, 0, tiled=True, axis_index_groups=pairs)
    chip = (halves[0].astype(jnp.float32) + halves[1].astype(jnp.float32)).astype(jnp.bfloat16)
    column_sum = lax.psum_scatter(chip, "gx", scatter_dimension=0, tiled=True)
    swapped = jnp.transpose(column_sum, (1, 0, 2, 3))
    beams = lax.psum_scatter(
        swapped, "gy", scatter_dimension=0, axis_index_groups=evens, tiled=True
    )
    power = detect(beams.reshape(runs // across, groups, beams_here, lanes))
    width = NCH // (across * along)
    order = channel_order[column]
    return jnp.take(power.reshape(beams_here, TIMES, along, width), order, axis=2).reshape(
        beams_here, TIMES, along * width
    )


def solution(mesh):
    return jax.shard_map(
        body,
        mesh=mesh,
        in_specs=(P(None, ("gx", "gy"), None), P(None, ("gx", "gy"), None), P(), P(), P()),
        out_specs=P("gy", None, "gx"),
        check_vma=False,
    )
```

```python
import functools
import math

import jax
import jax.numpy as jnp
from jax import lax
from jax.experimental import pallas as pl
from jax.experimental.pallas import tpu as pltpu
from jax.sharding import PartitionSpec as P

NIN = 2048
NCH = 8192
NBEAM = 64
TAPS = 8
INTEG = 2
NSPEC = 8
TIMES = 4
CHUNKS = 2
PITCH = 24
SLOT = 64
FIRST = 64
RUN = 64


def coefficients():
    total = TAPS * NCH
    index = jnp.arange(total, dtype=jnp.float32)
    offset = (index - total / 2) / NCH
    window = 0.5 - 0.5 * jnp.cos(2.0 * math.pi * index / total)
    raw = jnp.sinc(offset) * window
    raw = raw / jnp.sqrt(jnp.sum(raw * raw) / NCH)
    return raw.reshape(TAPS, NCH)


def combine_tables():
    second_len = NCH // FIRST
    first_ids = jnp.arange(FIRST, dtype=jnp.int32)
    second_ids = jnp.arange(second_len, dtype=jnp.int32)
    small = (2.0 * math.pi / FIRST) * (
        first_ids[:, None] * first_ids[None, :] % FIRST
    ).astype(jnp.float32)
    twist = (2.0 * math.pi / NCH) * (second_ids[:, None] * first_ids[None, :]).astype(jnp.float32)
    small_cos, small_sin = jnp.cos(small)[None], jnp.sin(small)[None]
    twist_cos, twist_sin = jnp.cos(twist)[:, :, None], jnp.sin(twist)[:, :, None]
    first = jnp.concatenate(
        [
            small_cos * twist_cos - small_sin * twist_sin,
            -(small_sin * twist_cos + small_cos * twist_sin),
        ],
        axis=2,
    ).astype(jnp.bfloat16)
    large = (2.0 * math.pi / second_len) * (
        second_ids[:, None] * second_ids[None, :] % second_len
    ).astype(jnp.float32)
    second = jnp.concatenate([jnp.cos(large), -jnp.sin(large)], axis=1).astype(jnp.bfloat16)
    return first, second


def filter_kernel(*refs):
    frames = refs[: NSPEC + TAPS - 1]
    taps = refs[NSPEC + TAPS - 1]
    out = refs[NSPEC + TAPS]
    inputs_here = frames[0].shape[1]
    for piece in range(out.shape[1]):
        lanes = slice(piece * 128, piece * 128 + 128)
        for spectrum in range(NSPEC):
            parts = []
            for part in range(2):
                total = taps[0:1, lanes] * frames[spectrum][part, :, lanes].astype(jnp.float32)
                for tap in range(1, TAPS):
                    total = total + taps[tap : tap + 1, lanes] * frames[spectrum + tap][
                        part, :, lanes
                    ].astype(jnp.float32)
                parts.append(total)
                if inputs_here < SLOT:
                    parts.append(jnp.zeros((SLOT - inputs_here, 128), jnp.float32))
            rows = jnp.concatenate(parts, axis=0)
            out[spectrum, piece] = jnp.transpose(rows).astype(jnp.bfloat16)


def quarter_turn(rows, sign):
    return pltpu.roll(rows, SLOT, 1) * sign


def lane_sign(count):
    lane = lax.broadcasted_iota(jnp.int32, (count, 2 * SLOT), 1)
    return jnp.where(lane < SLOT, -1.0, 1.0).astype(jnp.float32)


def first_kernel(rows, table, out, held):
    sign = lane_sign(FIRST)

    def hold(spectrum, carry):
        for term in range(FIRST):
            held[spectrum, term * PITCH : term * PITCH + 16] = rows[spectrum, term].astype(
                jnp.float32
            )
        return carry

    lax.fori_loop(0, NSPEC, hold, 0)
    for place in range(16):
        columns = []
        for spectrum in range(NSPEC):
            picked = held[spectrum, pl.ds(place, FIRST, stride=PITCH), :]
            columns.append(
                jnp.concatenate([picked, quarter_turn(picked, sign)], axis=0).astype(jnp.bfloat16)
            )
        sums = jnp.dot(
            table[place],
            jnp.concatenate(columns, axis=1),
            preferred_element_type=jnp.float32,
        ).astype(jnp.bfloat16)
        for spectrum in range(NSPEC):
            out[spectrum, place] = sums[:, spectrum * 128 : spectrum * 128 + 128]


def second_kernel(rows, table, gains, out, held, scales):
    second_len = NCH // FIRST
    sign = lane_sign(second_len)
    low = sign < 0.0
    for place in range(16):
        gain = gains[place] * NCH ** (-0.5)
        other = pltpu.roll(gain, SLOT, 1)
        scales[0, place] = jnp.where(low, gain, other)
        scales[1, place] = jnp.where(low, -other, gain)

    def spectrum_step(spectrum, carry):
        for term in range(second_len):
            held[term * PITCH : term * PITCH + 16] = rows[spectrum, term].astype(jnp.float32)
        for pair in range(8):
            columns = []
            for place in (2 * pair, 2 * pair + 1):
                picked = held[pl.ds(place, second_len, stride=PITCH), :]
                columns.append(
                    jnp.concatenate([picked, quarter_turn(picked, sign)], axis=0).astype(
                        jnp.bfloat16
                    )
                )
            sums = jnp.dot(
                table[...],
                jnp.concatenate(columns, axis=1),
                preferred_element_type=jnp.float32,
            )
            for inner in range(2):
                place = 2 * pair + inner
                value = sums[:, inner * 128 : inner * 128 + 128]
                out[place, spectrum] = (
                    value * scales[0, place] + pltpu.roll(value, SLOT, 1) * scales[1, place]
                ).astype(jnp.bfloat16)
        return carry

    lax.fori_loop(0, NSPEC, spectrum_step, 0)


def spectra_of(voltages, gains):
    inputs_here = voltages.shape[1]
    second_len = NCH // FIRST
    frames = NSPEC + TAPS - 1
    chunk = 2 * second_len
    chunks = NCH // chunk
    lanes = 2 * SLOT
    first, second = combine_tables()
    params = pltpu.CompilerParams(
        dimension_semantics=("arbitrary",), vmem_limit_bytes=48 * 1024 * 1024
    )
    filtered = pl.pallas_call(
        filter_kernel,
        grid=(chunks,),
        in_specs=[
            pl.BlockSpec((2, inputs_here, chunk), lambda step, frame=frame: (0, 0, frame * chunks + step))
            for frame in range(frames)
        ]
        + [pl.BlockSpec((TAPS, chunk), lambda step: (0, step))],
        out_specs=pl.BlockSpec((NSPEC, 2, second_len, lanes), lambda step: (0, step, 0, 0)),
        out_shape=jax.ShapeDtypeStruct((NSPEC, FIRST, second_len, lanes), jnp.bfloat16),
        compiler_params=params,
        name="fir",
    )(*([voltages] * frames), coefficients())
    turned = pl.pallas_call(
        first_kernel,
        grid=(second_len // 16,),
        in_specs=[
            pl.BlockSpec((NSPEC, FIRST, 16, lanes), lambda step: (0, 0, step, 0)),
            pl.BlockSpec((16, FIRST, 2 * FIRST), lambda step: (step, 0, 0)),
        ],
        out_specs=pl.BlockSpec((NSPEC, 16, FIRST, lanes), lambda step: (0, step, 0, 0)),
        out_shape=jax.ShapeDtypeStruct((NSPEC, second_len, FIRST, lanes), jnp.bfloat16),
        scratch_shapes=[pltpu.VMEM((NSPEC, FIRST * PITCH, lanes), jnp.float32)],
        compiler_params=params,
        name="first_sums",
    )(filtered, first)
    arranged = jnp.transpose(
        gains.reshape(2, inputs_here, second_len, FIRST), (3, 2, 0, 1)
    )
    if inputs_here < SLOT:
        arranged = jnp.pad(arranged, ((0, 0), (0, 0), (0, 0), (0, SLOT - inputs_here)))
    return pl.pallas_call(
        second_kernel,
        grid=(FIRST // 16,),
        in_specs=[
            pl.BlockSpec((NSPEC, second_len, 16, lanes), lambda step: (0, 0, step, 0)),
            pl.BlockSpec((second_len, 2 * second_len), lambda step: (0, 0)),
            pl.BlockSpec((16, second_len, lanes), lambda step: (step, 0, 0)),
        ],
        out_specs=pl.BlockSpec((16, NSPEC, second_len, lanes), lambda step: (step, 0, 0, 0)),
        out_shape=jax.ShapeDtypeStruct((FIRST, NSPEC, second_len, lanes), jnp.bfloat16),
        scratch_shapes=[pltpu.VMEM((second_len * PITCH, lanes), jnp.float32),
            pltpu.VMEM((2, 16, second_len, lanes), jnp.float32),
        ],
        compiler_params=params,
        name="second_sums",
    )(turned, second, arranged.reshape(FIRST, second_len, lanes))


def phase_tables(offsets):
    turn = offsets * (2.0 * math.pi / NCH)
    both = jnp.concatenate([turn, turn], axis=1)
    eight = jnp.arange(8, dtype=jnp.float32)
    near = eight[:, None, None] * both[None]
    near_cos, near_sin = jnp.cos(near)[:, None], jnp.sin(near)[:, None]
    far = (FIRST * eight)[:, None, None] * both[None]
    far_cos, far_sin = jnp.cos(far)[None], jnp.sin(far)[None]
    fine = jnp.stack(
        [near_cos * far_cos - near_sin * far_sin, near_sin * far_cos + near_cos * far_sin]
    ).reshape(2, RUN, NBEAM, 2 * SLOT)
    middle = (8.0 * jnp.arange(FIRST // 8, dtype=jnp.float32))[:, None, None] * both[None]
    blocks = NCH // FIRST // 8
    wide = (8.0 * FIRST * jnp.arange(blocks, dtype=jnp.float32))[:, None, None] * turn[None]
    wide_cos = jnp.cos(wide)
    wide_sin = jnp.sin(wide)
    scale = NIN ** (-0.5)
    return (
        fine,
        jnp.stack([jnp.cos(middle), jnp.sin(middle)]),
        jnp.stack(
            [
                jnp.concatenate([wide_cos, wide_sin], axis=2) * scale,
                jnp.concatenate([wide_sin, -wide_cos], axis=2) * scale,
            ]
        ),
    )


def beam_kernel(step, spectra, fine, middle, wide, out):
    lanes = 2 * SLOT
    bases = []
    for half in range(2):
        coarse = 2 * (step // (FIRST // 8)) + half
        rest = step % (FIRST // 8)
        wide_cos = wide[0, coarse]
        wide_sin = wide[1, coarse]
        middle_cos = middle[0, rest]
        middle_sin = middle[1, rest]
        bases.append(
            (
                wide_cos * middle_cos - wide_sin * middle_sin,
                wide_sin * middle_cos + wide_cos * middle_sin,
            )
        )
    lane = lax.broadcasted_iota(jnp.int32, (NBEAM, 2 * lanes), 1)
    member = lane % 8
    sign = jnp.where(
        lax.broadcasted_iota(jnp.int32, (8 * NSPEC, lanes), 1) < SLOT, 1.0, -1.0
    ).astype(jnp.float32)
    blank = jnp.zeros((16 * NSPEC, lanes), jnp.bfloat16)

    def group(index):
        rights = []
        both = spectra[index].astype(jnp.float32)
        for half in range(2):
            block = both[:, half * 8 : half * 8 + 8].reshape(8 * NSPEC, lanes)
            swapped = pltpu.roll(block, SLOT, 1) * sign
            rights.append(jnp.concatenate([block, swapped], axis=0).astype(jnp.bfloat16))
        right = jnp.concatenate(
            [
                jnp.concatenate([rights[0], blank], axis=1),
                jnp.concatenate([blank, rights[1]], axis=1),
            ],
            axis=0,
        )
        lefts = []
        for inner in range(8):
            fine_cos = fine[0, index * 8 + inner]
            fine_sin = fine[1, index * 8 + inner]
            lefts.append(
                jnp.concatenate(
                    [
                        (base_cos * fine_cos - base_sin * fine_sin).astype(jnp.bfloat16)
                        for base_cos, base_sin in bases
                    ],
                    axis=1,
                )
            )
        products = lax.dot_general(
            jnp.concatenate(lefts, axis=0),
            right,
            (((1,), (1,)), ((), ())),
            preferred_element_type=jnp.float32,
        )
        total = products[:NBEAM]
        for inner in range(1, 8):
            total = jnp.where(
                member == inner, products[inner * NBEAM : (inner + 1) * NBEAM], total
            )
        return total

    def pair(index, carry):
        low = group(2 * index)
        high = group(2 * index + 1)
        for unit in range(8):
            rows = slice(unit * 8, unit * 8 + 8)
            both = jnp.concatenate([low[rows], high[rows]], axis=0).astype(jnp.bfloat16)
            out[unit % 2, 0, unit // 2, pl.ds(index * 16, 16), :] = both
        return carry

    lax.fori_loop(0, RUN // 16, pair, 0, unroll=4)


def partial_beams(spectra, tables, across, chunk, chunks):
    share = NCH // (2 * RUN) // across // chunks
    runs = share * across
    fine, middle, wide = tables
    whole = lambda array: pl.BlockSpec(array.shape, lambda step: (0,) * array.ndim)

    def run_of(step):
        return step // share * (share * chunks) + chunk * share + step % share

    def kernel(spectra, fine, middle, wide, out):
        beam_kernel(run_of(pl.program_id(0)), spectra, fine, middle, wide, out)

    return pl.pallas_call(
        kernel,
        grid=(runs,),
        in_specs=[
            pl.BlockSpec(
                (8, NSPEC, 16, 2 * SLOT),
                lambda step: (run_of(step) % (FIRST // 8), 0, run_of(step) // (FIRST // 8), 0),
            ),
            whole(fine),
            whole(middle),
            whole(wide),
        ],
        out_specs=pl.BlockSpec((2, 1, 4, RUN, 4 * SLOT), lambda step: (0, step, 0, 0, 0)),
        out_shape=jax.ShapeDtypeStruct((2, runs, 4, RUN, 4 * SLOT), jnp.bfloat16),
        compiler_params=pltpu.CompilerParams(
            dimension_semantics=("arbitrary",), vmem_limit_bytes=48 * 1024 * 1024
        ),
        cost_estimate=pl.CostEstimate(
            flops=2 * runs * RUN * NBEAM * 256 * 256,
            bytes_accessed=runs * RUN * (2 * 8 + 4 * 8) * 2 * SLOT * 2,
            transcendentals=0,
        ),
        name="beam_sums",
    )(spectra, fine, middle, wide)


def detect(beams):
    runs, groups, count, lanes = beams.shape
    wide = beams.astype(jnp.bfloat16).astype(jnp.float32)
    source = jnp.arange(lanes, dtype=jnp.int32)
    source_half = source // (16 * NSPEC)
    source_channel = source % 8
    source_time = source // 8 % NSPEC // INTEG
    place = (source_half * TIMES + source_time) * 8 + source_channel
    pick = (place[:, None] == jnp.arange(2 * TIMES * 8, dtype=jnp.int32)[None]).astype(jnp.float32)
    power = jnp.einsum(
        "tgrl,lm->tgrm",
        wide * wide,
        pick,
        precision=lax.Precision.HIGHEST,
        preferred_element_type=jnp.float32,
    )
    parts = FIRST // 8
    power = power.reshape(runs // parts, parts, groups, count, 2, TIMES, 8)
    return jnp.transpose(power, (3, 5, 0, 4, 6, 1, 2)).reshape(count, TIMES, runs * 2 * groups * 8)


def body(voltages, gains, delays, channel_order, beam_table):
    across = lax.axis_size("gx")
    along = lax.axis_size("gy")
    inputs_here = voltages.shape[1]
    beams_here = NBEAM // along
    column = lax.axis_index("gx")
    member = lax.axis_index("gy")
    first_input = (column * along + member) * inputs_here
    offsets = jnp.take(
        lax.dynamic_slice_in_dim(delays, first_input, inputs_here, 1), beam_table, axis=0
    )
    if inputs_here < SLOT:
        offsets = jnp.pad(offsets, ((0, 0), (0, SLOT - inputs_here)))
    spectra = spectra_of(voltages, gains)
    tables = phase_tables(offsets)
    groups = RUN // 8
    lanes = 4 * SLOT
    pairs = [[2 * index, 2 * index + 1] for index in range(along // 2)]
    evens = [[2 * index + odd for index in range(along // 2)] for odd in range(2)]
    chunks = CHUNKS

    def exchange(share):
        return lax.all_to_all(share, "gy", 0, 0, tiled=True, axis_index_groups=evens)

    shares = []
    pieces = []
    for chunk in range(chunks):
        held_back = [shares[chunk - 2]] if chunk >= 2 else []
        held_back += [pieces[chunk - 3]] if chunk >= 3 else []
        tables, held_back = lax.optimization_barrier((tables, held_back))
        if chunk >= 2:
            shares[chunk - 2] = held_back[0]
            pieces.append(exchange(shares[chunk - 2]))
        if chunk >= 3:
            pieces[chunk - 3] = held_back[1]
        partial = partial_beams(spectra, tables, across, chunk, chunks)
        runs = partial.shape[1]
        if beams_here != 8:
            partial = jnp.transpose(
                partial.reshape(2, runs, 4, groups, 8, lanes), (2, 0, 4, 1, 3, 5)
            ).reshape(along // 2, 2, beams_here, runs, groups, lanes)
            partial = jnp.transpose(partial, (1, 3, 0, 4, 2, 5)).reshape(
                2, runs, along // 2, groups * beams_here, lanes
            )
        halves = lax.all_to_all(partial, "gy", 0, 0, tiled=True, axis_index_groups=pairs)
        chip = (halves[0].astype(jnp.float32) + halves[1].astype(jnp.float32)).astype(jnp.bfloat16)
        column_sum = lax.psum_scatter(chip, "gx", scatter_dimension=0, tiled=True)
        shares.append(jnp.transpose(column_sum, (1, 0, 2, 3)))
    pieces += [exchange(share) for share in shares[len(pieces) :]]
    beams = jnp.concatenate([piece.astype(jnp.float32).sum(axis=0) for piece in pieces], axis=0)
    power = detect(beams.reshape(-1, groups, beams_here, lanes))
    width = NCH // (across * along)
    order = channel_order[column]
    return jnp.take(power.reshape(beams_here, TIMES, along, width), order, axis=2).reshape(
        beams_here, TIMES, along * width
    )


def solution(mesh):
    return jax.shard_map(
        body,
        mesh=mesh,
        in_specs=(P(None, ("gx", "gy"), None), P(None, ("gx", "gy"), None), P(), P(), P()),
        out_specs=P("gy", None, "gx"),
        check_vma=False,
    )
```
